32 devices in a mesh: blk: 16 (over z, x, core), pair: 2 (over y).
Axes of the slice: x: 2, y: 2, z: 4, core: 2. Of those that a mesh axis runs over, the one named last changes fastest.
Arguments:
- vertex: bfloat16 [16, 2048, 2048], P('blk', 'pair'), may hold values from -0.125 to 0.125
- left_phase: bfloat16 [16, 2048, 512], P('blk', 'pair'), may hold values from -6 to 6
- right_phase: bfloat16 [16, 2048, 512], P('blk'), may hold values from -6 to 6
- tiles: bfloat16 [64, 512, 512], P('blk'), may hold values from -0.25 to 0.25
- orders: int32 [16], P('blk'), may hold values from 512 to 2048, as said below
- momentum: int32 [512], replicated, may hold values from 0 to 63
- frequency: int32 [512], replicated, may hold values from 0 to 31
Outputs:
- suscept: bfloat16 [64, 512, 512], P('blk', 'pair')
- sigma: float32 [2048], P(('blk', 'pair'))
The draws below stay inside these ranges and needn't reach their ends.
Inputs may be any that keep to these rules, and one draw needn't show every extreme that they name: `orders`: every order is at least 512 and at most 2048; some walker has order exactly 2048.
All inputs are finite; a program needn't handle non-finite values.
Results may differ from the reference program's by a relative error of at most 0.0075.
Values may be sent and summed in bfloat16 or wider, within the bound.
A program may use at most 64 MiB of HBM per device.

```python
import math
import jax
import jax.numpy as jnp
from jax import lax

S = 512
KMAX = 2048
TILES_DEV = 4
NMOM = 64
NFREQ = 32
WALKERS = 16
TILES = 64
N_BLK = 16


def draw_orders(key, part):
    values = jax.random.randint(key, (WALKERS,), KMAX // 4, KMAX + 1)
    chosen = jax.random.randint(jax.random.fold_in(key, 7), (), 0, WALKERS)
    return values.at[chosen].set(KMAX).astype(jnp.int32)


def touch_ends(array, stream_key, smallest, largest):
    longest = array.shape.index(max(array.shape))
    spots = []
    for shift in (0, 1):
        where = [jax.random.randint(jax.random.fold_in(stream_key, axis), (), 0, length) for axis, length in enumerate(array.shape)]
        where[longest] = (where[longest] + shift) % array.shape[longest]
        spots.append(tuple(where))
    return array.at[spots[0]].set(smallest).at[spots[1]].set(largest)


def block_scale(own_key, extent, split, low, largest):
    def one(position, shards_of):
        heights = jax.random.uniform(jax.random.fold_in(jax.random.fold_in(own_key, 6), position), (shards_of,), jnp.float32, low / len(split), largest / len(split))
        return jnp.repeat(jnp.exp(heights), extent[position] // shards_of).reshape((-1,) + (1,) * (len(extent) - position - 1))

    loudness = one(*split[0])
    for cut in split[1:]:
        loudness = loudness * one(*cut)
    return loudness


def normal_values(rng, extent, width, limit, split=(), kind=jnp.bfloat16):
    gain = block_scale(rng, extent, split, -0.22, 0.18) if split else 1.0
    values = jax.random.normal(rng, extent, jnp.float32) * width * gain
    return jnp.minimum(jnp.maximum(values, -limit), limit).astype(kind)


def setup_inputs(seed: int = 0) -> dict:
    seeds = jax.random.split(jax.random.key(seed), 8)
    return {
        "vertex": normal_values(seeds[0], (WALKERS, KMAX, KMAX), KMAX ** -0.5, 0.125, ((0, 16), (1, 2))),
        "left_phase": normal_values(seeds[1], (WALKERS, KMAX, S), 1.0, 6.0, ((0, 16), (1, 2))),
        "right_phase": normal_values(seeds[2], (WALKERS, KMAX, S), 1.0, 6.0, ((0, 16),)),
        "tiles": normal_values(seeds[3], (TILES, S, S), S ** -0.5, 0.25, ((0, 16),)),
        "orders": draw_orders(jax.random.fold_in(seeds[7], 71), 0),
        "momentum": touch_ends(jax.random.randint(seeds[5], (S,), 0, NMOM), jax.random.fold_in(seeds[5], 1), 0, NMOM - 1).astype(jnp.int32),
        "frequency": touch_ends(jax.random.randint(seeds[6], (S,), 0, NFREQ), jax.random.fold_in(seeds[6], 1), 0, NFREQ - 1).astype(jnp.int32),
    }


def reference(vertex, left_phase, right_phase, tiles, orders, momentum, frequency):
    positions = jnp.arange(KMAX, dtype=jnp.int32)

    def one_walker(items):
        matrix, left, right, order = items
        live = positions < order
        masked = jnp.where(live[:, None] & live[None, :], matrix, jnp.zeros_like(matrix))
        carried = jnp.dot(masked, right, preferred_element_type=jnp.float32).astype(jnp.bfloat16)
        green = lax.dot_general(left, carried, (((0,), (0,)), ((), ())), preferred_element_type=jnp.float32)
        return (green / math.sqrt(KMAX)).astype(jnp.bfloat16)
    greens = lax.map(one_walker, (vertex, left_phase, right_phase, orders))
    grouped = tiles.reshape(N_BLK, TILES_DEV, S, S)
    onehot_mom = (momentum[:, None] == jnp.arange(NMOM, dtype=jnp.int32)[None, :]).astype(jnp.float32)
    onehot_freq = (frequency[:, None] == jnp.arange(NFREQ, dtype=jnp.int32)[None, :]).astype(jnp.float32)
    offsets = jnp.arange(-2, 3, dtype=jnp.int32)

    def one_block(number):
        window = jnp.take(greens, (number + offsets) % N_BLK, axis=0).astype(jnp.float32)
        block_tiles = grouped[number].astype(jnp.float32)
        inner = jnp.einsum('usa,tab->utsb', window, block_tiles).astype(jnp.bfloat16).astype(jnp.float32)
        chi = jnp.einsum('utsb,ucb->tsc', inner, window) / math.sqrt(S)
        summed = lax.optimization_barrier(jnp.sum(chi, axis=0))
        partial_value = jnp.dot(summed, onehot_freq, precision=lax.Precision.HIGHEST)
        cells = jnp.dot(onehot_mom.T, partial_value, precision=lax.Precision.HIGHEST)
        return (chi.astype(jnp.bfloat16), cells)
    chis, cells = lax.map(one_block, jnp.arange(N_BLK, dtype=jnp.int32))
    factor = 1.0 / math.sqrt(5.0 * TILES_DEV * N_BLK * S * S / (NMOM * NFREQ))
    sigma = (lax.optimization_barrier(jnp.sum(cells, axis=0)) * factor).reshape(-1)
    return (chis.reshape(TILES_DEV * N_BLK, S, S), sigma)
```

```python
import math

import jax
import jax.numpy as jnp
from jax import lax
from jax.experimental import pallas as pl
from jax.experimental.pallas import tpu as pltpu
from jax.sharding import PartitionSpec as P

NMOM = 64
NFREQ = 32
LANES = 128
CHUNKS = 8
MESH = pl.DeviceIdType.MESH
OWN, PEER, ACROSS, RELAYED, FORWARDED = range(5)


def contract(a, b, dims, precision=None):
    return lax.dot_general(
        a, b, (dims, ((), ())), preferred_element_type=jnp.float32, precision=precision
    )


def body(sizes, order_ref, mom_ref, freq_ref, vertex_hbm, left_hbm, right_hbm, tiles_hbm,
         out_ref, sigma_ref,
         vertex, left, right, tiles, carried, partial, sending, arrived, greens, inner, acc,
         cells_ref, sig_send, sig_recv, load_sem, y_send, y_recv, x_send, x_recv, z_send, z_recv,
         p_send, p_recv, f_send, f_recv, s_send, s_recv):
    n_blk, n_pair, height, breadth, states, n_tiles = sizes
    count = n_blk * n_pair
    half = states // n_pair
    b = lax.axis_index("blk")
    p = lax.axis_index("pair")
    me = b * n_pair + p
    chip = b // 2
    core = lax.rem(b, 2)
    odd = lax.rem(chip, 2)
    step = 1 - 2 * odd
    across = (lax.rem(b + 2 * step + n_blk, n_blk), p)
    along = (lax.rem(b + 4 * step + n_blk, n_blk), p)
    peer = (b + 1 - 2 * core, p)
    other = (b, 1 - p)
    forwards_across = lax.rem(odd + core, 2) == 0

    barrier = pltpu.get_barrier_semaphore()

    def greet(i, carry):
        to = lax.rem(me + i, count)
        pl.semaphore_signal(barrier, inc=1, device_id=(to // n_pair, lax.rem(to, n_pair)),
                            device_id_type=MESH)
        return carry

    lax.fori_loop(1, count, greet, 0)

    pieces = 4
    block = height // pieces
    load_right = pltpu.make_async_copy(right_hbm.at[0], right, load_sem.at[0])
    load_right.start()
    load_vertex = []
    for i in range(pieces):
        rows = pl.ds(i * block, block)
        copy = pltpu.make_async_copy(vertex_hbm.at[0, rows], vertex.at[rows], load_sem.at[1 + i])
        copy.start()
        load_vertex.append(copy)
    load_left = pltpu.make_async_copy(left_hbm.at[0], left, load_sem.at[1 + pieces])
    load_left.start()
    load_tiles = pltpu.make_async_copy(tiles_hbm, tiles, load_sem.at[2 + pieces])
    load_tiles.start()

    order = order_ref[0]
    load_right.wait()

    def mask_right(i, carry):
        rows = pl.ds(pl.multiple_of(i * 256, 256), 256)
        ids = i * 256 + lax.broadcasted_iota(jnp.int32, (256, states), 0)
        right[rows, :] = jnp.where(ids < order, right[rows, :], jnp.zeros((), jnp.bfloat16))
        return carry

    lax.fori_loop(0, breadth // 256, mask_right, 0)

    for i in range(pieces):
        load_vertex[i].wait()
        rows = pl.ds(i * block, block)
        product = contract(vertex[rows, :], right[...], ((1,), (0,)))
        ids = p * height + i * block + lax.broadcasted_iota(jnp.int32, (block, states), 0)
        carried[rows, :] = jnp.where(ids < order, product, 0.0).astype(jnp.bfloat16)

    load_left.wait()
    pl.semaphore_wait(barrier, count - 1)

    scale = 1.0 / math.sqrt(breadth)
    size = states // CHUNKS
    per_half = half // size

    def chunk(which, k):
        return pl.ds(pl.multiple_of(lax.rem(which * per_half + k, CHUNKS) * size, size), size)

    def exchange(k):
        rows = chunk(1 - p, k)
        return pltpu.make_async_remote_copy(
            src_ref=sending.at[rows], dst_ref=arrived.at[rows], send_sem=y_send.at[k],
            recv_sem=y_recv.at[k], device_id=other, device_id_type=MESH)

    def arrival(k):
        rows = chunk(p, k)
        return pltpu.make_async_remote_copy(
            src_ref=sending.at[rows], dst_ref=arrived.at[rows], send_sem=y_send.at[k],
            recv_sem=y_recv.at[k], device_id=other, device_id_type=MESH)

    def hop(source, target, k, send, recv, device):
        rows = chunk(p, k)
        return pltpu.make_async_remote_copy(
            src_ref=greens.at[source, rows], dst_ref=greens.at[target, rows], send_sem=send.at[k],
            recv_sem=recv.at[k], device_id=device, device_id_type=MESH)

    def to_across(k):
        return hop(OWN, ACROSS, k, x_send, x_recv, across)

    def to_peer(k):
        return hop(OWN, PEER, k, p_send, p_recv, peer)

    def to_along(k):
        return hop(ACROSS, RELAYED, k, z_send, z_recv, along)

    def forward(source, k):
        return hop(source, FORWARDED, k, f_send, f_recv, peer)

    for part in range(n_pair):
        which = lax.rem(1 - p + part, n_pair)
        first = pl.multiple_of(which * half, half)
        rows = pl.ds(first, half)
        product = contract(left[:, rows], carried[...], ((0,), (0,))) * scale
        partial[rows, :] = product
        sending[rows, :] = product.astype(jnp.bfloat16)
        for k in range(per_half):
            exchange(part * per_half + k).start()

    ids_m = lax.broadcasted_iota(jnp.int32, (NMOM, half), 0)
    pick_mom = (ids_m == mom_ref[p]).astype(jnp.bfloat16)
    ids_f = lax.broadcasted_iota(jnp.int32, (LANES, states), 0)
    pick_freq = (ids_f == freq_ref[...]).astype(jnp.bfloat16)
    own_rows = pl.ds(pl.multiple_of(p * half, half), half)

    def compute_inner(slot, slot_index):
        upper = greens[slot, own_rows, :]
        total = jnp.zeros((half, states), jnp.float32)
        for t in range(n_tiles):
            value = contract(upper, tiles[t], ((1,), (0,))).astype(jnp.bfloat16)
            inner[slot_index, pl.ds(t * half, half), :] = value
            total = total + value.astype(jnp.float32)
        high = total.astype(jnp.bfloat16)
        low = (total - high.astype(jnp.float32)).astype(jnp.bfloat16)
        return contract(pick_mom, high, ((1,), (0,))) + contract(pick_mom, low, ((1,), (0,)))

    def compute_cells(slot, folded, first=False):
        picked = contract(pick_freq, greens[slot], ((1,), (0,)))
        value = contract(folded, picked, ((1,), (1,)), lax.Precision.HIGHEST)
        cells_ref[...] = value if first else cells_ref[...] + value

    out_scale = 1.0 / math.sqrt(states)

    def compute_chi(slot, slot_index, first=False, last=False):
        for t in range(n_tiles):
            rows = pl.ds(t * half, half)
            value = contract(inner[slot_index, rows, :], greens[slot], ((1,), (1,)))
            if not first:
                value = acc[rows, :] + value
            if last:
                out_ref[t] = (value * out_scale).astype(jnp.bfloat16)
            else:
                acc[rows, :] = value

    def take_y(k):
        arrival(k).wait_recv()
        rows = chunk(p, k)
        greens[OWN, rows, :] = (
            partial[rows, :] + arrived[rows, :].astype(jnp.float32)
        ).astype(jnp.bfloat16)
        to_across(k).start()
        to_peer(k).start()

    def take_x(k):
        to_across(k).wait_recv()
        to_along(k).start()

        @pl.when(forwards_across)
        def _():
            forward(ACROSS, k).start()

    def take_z(k):
        to_along(k).wait_recv()

        @pl.when(jnp.logical_not(forwards_across))
        def _():
            forward(RELAYED, k).start()

    folds = {}
    lag = 2
    for s in range(CHUNKS + 2 * lag):
        if s < CHUNKS:
            take_y(s)
        if 0 <= s - lag < CHUNKS:
            take_x(s - lag)
        if 0 <= s - 2 * lag < CHUNKS:
            take_z(s - 2 * lag)
        if s == per_half - 1:
            load_tiles.wait()
            folds[OWN] = compute_inner(OWN, 0)
        if s == per_half + 1:
            for k in range(per_half):
                to_peer(k).wait_recv()
            folds[PEER] = compute_inner(PEER, 1)
        if s == per_half + 2:
            folds[ACROSS] = compute_inner(ACROSS, 2)
        if s == CHUNKS - 1:
            compute_cells(OWN, folds[OWN], first=True)
            compute_chi(OWN, 0, first=True)
        if s == CHUNKS:
            folds[RELAYED] = compute_inner(RELAYED, 3)
        if s == CHUNKS + 1:
            for k in range(per_half, CHUNKS):
                to_peer(k).wait_recv()
            compute_cells(PEER, folds[PEER])
            compute_chi(PEER, 1)
        if s == CHUNKS + 2:
            for k in range(per_half):
                forward(ACROSS, k).wait_recv()
            folds[FORWARDED] = compute_inner(FORWARDED, 4)
            compute_cells(ACROSS, folds[ACROSS])

    compute_cells(RELAYED, folds[RELAYED])
    for k in range(per_half, CHUNKS):
        forward(ACROSS, k).wait_recv()
    compute_cells(FORWARDED, folds[FORWARDED])

    own_cells = NMOM * NFREQ // count
    cells = cells_ref[...]
    rows_d = lax.broadcasted_iota(jnp.int32, (count, NMOM), 0)
    cols_m = lax.broadcasted_iota(jnp.int32, (count, NMOM), 1)
    spread = jnp.zeros((count, LANES), jnp.float32)
    if own_cells >= NFREQ:
        group = own_cells // NFREQ
        for k in range(group):
            pick = (cols_m == rows_d * group + k).astype(jnp.float32)
            value = contract(pick, cells, ((1,), (0,)), lax.Precision.HIGHEST)
            spread = spread + (pltpu.roll(value, NFREQ * k, 1) if k else value)
    else:
        group = NFREQ // own_cells
        for k in range(group):
            pick = (rows_d == cols_m * group + k).astype(jnp.float32)
            value = contract(pick, cells, ((1,), (0,)), lax.Precision.HIGHEST)
            spread = spread + (pltpu.roll(value, LANES - own_cells * k, 1) if k else value)
    factor = 1.0 / math.sqrt(5.0 * n_tiles * n_blk * states * states / (NMOM * NFREQ))
    spread = spread * (factor * out_scale)
    sig_send[...] = spread.reshape(count, 1, LANES)

    def owner(i):
        to = lax.rem(me + i, count)
        return pltpu.make_async_remote_copy(
            src_ref=sig_send.at[to], dst_ref=sig_recv.at[i - 1], send_sem=s_send.at[i - 1],
            recv_sem=s_recv.at[i - 1], device_id=(to // n_pair, lax.rem(to, n_pair)),
            device_id_type=MESH)

    def send_cells(i, carry):
        owner(i).start()
        return carry

    lax.fori_loop(1, count, send_cells, 0)

    compute_chi(ACROSS, 2)
    compute_chi(RELAYED, 3)
    compute_chi(FORWARDED, 4, last=True)

    for k in range(CHUNKS):
        exchange(k).wait_send()
        to_across(k).wait_send()
        to_peer(k).wait_send()
        to_along(k).wait_send()
        forward(ACROSS, k).wait_send()

    def take_cells(i, carry):
        owner(i).wait()
        return carry

    lax.fori_loop(1, count, take_cells, 0)
    sigma_ref[...] = jnp.sum(sig_recv[...], axis=0) + sig_send[me]


def solution(mesh):
    n_blk, n_pair = mesh.shape["blk"], mesh.shape["pair"]
    count = n_blk * n_pair

    def per_device(vertex, left_phase, right_phase, tiles, orders, momentum, frequency):
        height, breadth = vertex.shape[1], vertex.shape[2]
        states = right_phase.shape[2]
        n_tiles = tiles.shape[0]
        half = states // n_pair
        sizes = (n_blk, n_pair, height, breadth, states, n_tiles)
        bf16, f32 = jnp.bfloat16, jnp.float32
        dma = pltpu.SemaphoreType.DMA
        chi, cells = pl.pallas_call(
            lambda *refs: body(sizes, *refs),
            out_shape=(
                jax.ShapeDtypeStruct((n_tiles, half, states), bf16),
                jax.ShapeDtypeStruct((1, LANES), f32),
            ),
            in_specs=[
                pl.BlockSpec(memory_space=pltpu.SMEM),
                pl.BlockSpec(memory_space=pltpu.VMEM),
                pl.BlockSpec(memory_space=pltpu.VMEM),
            ] + [pl.BlockSpec(memory_space=pl.ANY)] * 4,
            out_specs=(
                pl.BlockSpec(memory_space=pltpu.VMEM),
                pl.BlockSpec(memory_space=pltpu.VMEM),
            ),
            scratch_shapes=[
                pltpu.VMEM((height, breadth), bf16),
                pltpu.VMEM((height, states), bf16),
                pltpu.VMEM((breadth, states), bf16),
                pltpu.VMEM((n_tiles, states, states), bf16),
                pltpu.VMEM((height, states), bf16),
                pltpu.VMEM((states, states), f32),
                pltpu.VMEM((states, states), bf16),
                pltpu.VMEM((states, states), bf16),
                pltpu.VMEM((5, states, states), bf16),
                pltpu.VMEM((5, n_tiles * half, states), bf16),
                pltpu.VMEM((n_tiles * half, states), f32),
                pltpu.VMEM((NMOM, LANES), f32),
                pltpu.VMEM((count, 1, LANES), f32),
                pltpu.VMEM((count - 1, 1, LANES), f32),
                dma((7,)),
            ] + [dma((CHUNKS,))] * 10 + [dma((count - 1,))] * 2,
            compiler_params=pltpu.CompilerParams(
                collective_id=0, has_side_effects=True, vmem_limit_bytes=60 * 1024 * 1024
            ),
            name="measure_green",
        )(
            orders,
            momentum.reshape(n_pair, 1, half),
            frequency.reshape(1, states),
            vertex,
            left_phase,
            right_phase,
            tiles,
        )
        own = NMOM * NFREQ // count
        return chi, cells[0, :own]

    in_specs = (
        P("blk", "pair", None),
        P("blk", "pair", None),
        P("blk", None, None),
        P("blk", None, None),
        P("blk"),
        P(),
        P(),
    )
    out_specs = (P("blk", "pair", None), P(("blk", "pair")))
    return jax.shard_map(
        per_device, mesh=mesh, in_specs=in_specs, out_specs=out_specs, check_vma=False
    )
```

```python
import math

import jax
import jax.numpy as jnp
from jax import lax
from jax.experimental import pallas as pl
from jax.experimental.pallas import tpu as pltpu
from jax.sharding import PartitionSpec as P

NMOM = 64
NFREQ = 32
LANES = 128
CHUNKS = 8
SPLIT = 2
MESH = pl.DeviceIdType.MESH
OWN, PEER, ACROSS, RELAYED, FORWARDED = range(5)


def contract(a, b, dims, precision=None):
    return lax.dot_general(
        a, b, (dims, ((), ())), preferred_element_type=jnp.float32, precision=precision
    )


def body(sizes, order_ref, mom_ref, freq_ref, vertex_hbm, left_hbm, right_hbm, tiles_hbm,
         out_ref, sigma_ref,
         vertex, left, right, tiles, carried, partial, sending, arrived, greens, inner, acc,
         cells_ref, sig_send, sig_recv, load_sem, y_send, y_recv, x_send, x_recv, z_send, z_recv,
         p_send, p_recv, f_send, f_recv, s_send, s_recv,
         chi, o_sem):
    n_blk, n_pair, height, breadth, states, n_tiles = sizes
    count = n_blk * n_pair
    half = states // n_pair
    b = lax.axis_index("blk")
    p = lax.axis_index("pair")
    me = b * n_pair + p
    chip = b // 2
    core = lax.rem(b, 2)
    odd = lax.rem(chip, 2)
    step = 1 - 2 * odd
    across = (lax.rem(b + 2 * step + n_blk, n_blk), p)
    along = (lax.rem(b + 4 * step + n_blk, n_blk), p)
    peer = (b + 1 - 2 * core, p)
    other = (b, 1 - p)
    forwards_across = lax.rem(odd + core, 2) == 0

    barrier = pltpu.get_barrier_semaphore()

    def greet(i, carry):
        to = lax.rem(me + i, count)
        pl.semaphore_signal(barrier, inc=1, device_id=(to // n_pair, lax.rem(to, n_pair)),
                            device_id_type=MESH)
        return carry

    lax.fori_loop(1, count, greet, 0)

    pieces = 4
    block = height // pieces
    wide = states // SPLIT

    def load_right(h):
        cols = pl.ds(h * wide, wide)
        return pltpu.make_async_copy(right_hbm.at[0, :, cols], right.at[h], load_sem.at[h])

    load_right(0).start()
    load_vertex = []
    for i in range(pieces):
        rows = pl.ds(i * block, block)
        copy = pltpu.make_async_copy(vertex_hbm.at[0, rows], vertex.at[rows], load_sem.at[SPLIT + i])
        copy.start()
        load_vertex.append(copy)
    load_left = pltpu.make_async_copy(left_hbm.at[0], left, load_sem.at[SPLIT + pieces])
    load_left.start()
    for h in range(1, SPLIT):
        load_right(h).start()
    load_tiles = pltpu.make_async_copy(tiles_hbm, tiles, load_sem.at[SPLIT + 1 + pieces])
    load_tiles.start()

    order = order_ref[0]
    scale = 1.0 / math.sqrt(breadth)
    per_split = CHUNKS // SPLIT
    size = states // per_split
    per_half = half // size

    def chunk(which, k):
        index = lax.rem(which * per_half + k % per_split, per_split)
        return (pl.ds(pl.multiple_of(index * size, size), size),
                pl.ds(k // per_split * wide, wide))

    def exchange(k):
        rows = chunk(1 - p, k)
        return pltpu.make_async_remote_copy(
            src_ref=sending.at[*rows], dst_ref=arrived.at[*rows], send_sem=y_send.at[k],
            recv_sem=y_recv.at[k], device_id=other, device_id_type=MESH)

    def arrival(k):
        rows = chunk(p, k)
        return pltpu.make_async_remote_copy(
            src_ref=sending.at[*rows], dst_ref=arrived.at[*rows], send_sem=y_send.at[k],
            recv_sem=y_recv.at[k], device_id=other, device_id_type=MESH)

    def hop(source, target, k, send, recv, device):
        rows = chunk(p, k)
        return pltpu.make_async_remote_copy(
            src_ref=greens.at[source, *rows], dst_ref=greens.at[target, *rows], send_sem=send.at[k],
            recv_sem=recv.at[k], device_id=device, device_id_type=MESH)

    def to_across(k):
        return hop(OWN, ACROSS, k, x_send, x_recv, across)

    def to_peer(k):
        return hop(OWN, PEER, k, p_send, p_recv, peer)

    def to_along(k):
        return hop(ACROSS, RELAYED, k, z_send, z_recv, along)

    def forward(source, k):
        return hop(source, FORWARDED, k, f_send, f_recv, peer)

    for h in range(SPLIT):
        load_right(h).wait()

        def mask_right(i, carry):
            rows = pl.ds(pl.multiple_of(i * 256, 256), 256)
            ids = i * 256 + lax.broadcasted_iota(jnp.int32, (256, wide), 0)
            right[h, rows, :] = jnp.where(ids < order, right[h, rows, :], jnp.zeros((), jnp.bfloat16))
            return carry

        lax.fori_loop(0, breadth // 256, mask_right, 0)
        for i in range(pieces):
            rows = pl.ds(i * block, block)
            if h == 0:
                load_vertex[i].wait()
            product = contract(vertex[rows, :], right[h], ((1,), (0,)))
            ids = p * height + i * block + lax.broadcasted_iota(jnp.int32, (block, wide), 0)
            carried[rows, :] = jnp.where(ids < order, product, 0.0).astype(jnp.bfloat16)
        if h == 0:
            load_left.wait()
            pl.semaphore_wait(barrier, count - 1)
        cols = pl.ds(h * wide, wide)
        for part in range(n_pair):
            which = lax.rem(1 - p + part, n_pair)
            rows = pl.ds(pl.multiple_of(which * half, half), half)
            product = contract(left[:, rows], carried[...], ((0,), (0,))) * scale
            partial[rows, cols] = product
            sending[rows, cols] = product.astype(jnp.bfloat16)
            for k in range(per_half):
                exchange(h * per_split + part * per_half + k).start()

    ids_m = lax.broadcasted_iota(jnp.int32, (NMOM, half), 0)
    pick_mom = (ids_m == mom_ref[p]).astype(jnp.bfloat16)
    ids_f = lax.broadcasted_iota(jnp.int32, (LANES, states), 0)
    pick_freq = (ids_f == freq_ref[...]).astype(jnp.bfloat16)
    own_rows = pl.ds(pl.multiple_of(p * half, half), half)

    def compute_inner(slot, slot_index):
        upper = greens[slot, own_rows, :]
        total = jnp.zeros((half, states), jnp.float32)
        for t in range(n_tiles):
            value = contract(upper, tiles[t], ((1,), (0,))).astype(jnp.bfloat16)
            inner[slot_index, pl.ds(t * half, half), :] = value
            total = total + value.astype(jnp.float32)
        high = total.astype(jnp.bfloat16)
        low = (total - high.astype(jnp.float32)).astype(jnp.bfloat16)
        return contract(pick_mom, high, ((1,), (0,))) + contract(pick_mom, low, ((1,), (0,)))

    def compute_cells(slot, folded, first=False):
        picked = contract(pick_freq, greens[slot], ((1,), (0,)))
        value = contract(folded, picked, ((1,), (1,)), lax.Precision.HIGHEST)
        cells_ref[...] = value if first else cells_ref[...] + value

    out_scale = 1.0 / math.sqrt(states)

    def store(t):
        return pltpu.make_async_copy(chi.at[t], out_ref.at[t], o_sem.at[t])

    def compute_chi(slot, slot_index, first=False, last=False):
        for t in range(n_tiles):
            rows = pl.ds(t * half, half)
            value = contract(inner[slot_index, rows, :], greens[slot], ((1,), (1,)))
            if not first:
                value = acc[rows, :] + value
            if last:
                chi[t] = (value * out_scale).astype(jnp.bfloat16)
                store(t).start()
            else:
                acc[rows, :] = value

    def take_y(k):
        arrival(k).wait_recv()
        rows = chunk(p, k)
        greens[OWN, *rows] = (
            partial[*rows] + arrived[*rows].astype(jnp.float32)
        ).astype(jnp.bfloat16)
        to_across(k).start()
        to_peer(k).start()

    def take_x(k):
        to_across(k).wait_recv()
        to_along(k).start()

        @pl.when(forwards_across)
        def _():
            forward(ACROSS, k).start()

    def take_z(k):
        to_along(k).wait_recv()

        @pl.when(jnp.logical_not(forwards_across))
        def _():
            forward(RELAYED, k).start()

    folds = {}
    upper_last = CHUNKS - per_split + per_half - 1
    lag = 2
    for s in range(CHUNKS + 2 * lag):
        if s < CHUNKS:
            take_y(s)
        if 0 <= s - lag < CHUNKS:
            take_x(s - lag)
        if 0 <= s - 2 * lag < CHUNKS:
            take_z(s - 2 * lag)
        if s == upper_last:
            load_tiles.wait()
            folds[OWN] = compute_inner(OWN, 0)
        if s == CHUNKS - 1:
            compute_cells(OWN, folds[OWN], first=True)
            compute_chi(OWN, 0, first=True)
        if s == CHUNKS:
            for k in range(CHUNKS):
                to_peer(k).wait_recv()
            folds[PEER] = compute_inner(PEER, 1)
            folds[ACROSS] = compute_inner(ACROSS, 2)
        if s == CHUNKS + 1:
            compute_cells(PEER, folds[PEER])
            compute_cells(ACROSS, folds[ACROSS])
        if s == CHUNKS + lag:
            folds[RELAYED] = compute_inner(RELAYED, 3)
            for k in range(upper_last + 1):
                forward(ACROSS, k).wait_recv()
            folds[FORWARDED] = compute_inner(FORWARDED, 4)

    compute_cells(RELAYED, folds[RELAYED])
    for k in range(upper_last + 1, CHUNKS):
        forward(ACROSS, k).wait_recv()
    compute_cells(FORWARDED, folds[FORWARDED])

    own_cells = NMOM * NFREQ // count
    cells = cells_ref[...]
    rows_d = lax.broadcasted_iota(jnp.int32, (count, NMOM), 0)
    cols_m = lax.broadcasted_iota(jnp.int32, (count, NMOM), 1)
    spread = jnp.zeros((count, LANES), jnp.float32)
    if own_cells >= NFREQ:
        group = own_cells // NFREQ
        for k in range(group):
            pick = (cols_m == rows_d * group + k).astype(jnp.float32)
            value = contract(pick, cells, ((1,), (0,)), lax.Precision.HIGHEST)
            spread = spread + (pltpu.roll(value, NFREQ * k, 1) if k else value)
    else:
        group = NFREQ // own_cells
        for k in range(group):
            pick = (rows_d == cols_m * group + k).astype(jnp.float32)
            value = contract(pick, cells, ((1,), (0,)), lax.Precision.HIGHEST)
            spread = spread + (pltpu.roll(value, LANES - own_cells * k, 1) if k else value)
    factor = 1.0 / math.sqrt(5.0 * n_tiles * n_blk * states * states / (NMOM * NFREQ))
    spread = spread * (factor * out_scale)
    sig_send[...] = spread.reshape(count, 1, LANES)

    def owner(i):
        to = lax.rem(me + i, count)
        return pltpu.make_async_remote_copy(
            src_ref=sig_send.at[to], dst_ref=sig_recv.at[i - 1], send_sem=s_send.at[i - 1],
            recv_sem=s_recv.at[i - 1], device_id=(to // n_pair, lax.rem(to, n_pair)),
            device_id_type=MESH)

    def send_cells(i, carry):
        owner(i).start()
        return carry

    lax.fori_loop(1, count, send_cells, 0)

    compute_chi(PEER, 1)
    compute_chi(ACROSS, 2)
    compute_chi(RELAYED, 3)
    compute_chi(FORWARDED, 4, last=True)

    for k in range(CHUNKS):
        exchange(k).wait_send()
        to_across(k).wait_send()
        to_peer(k).wait_send()
        to_along(k).wait_send()
        forward(ACROSS, k).wait_send()

    for t in range(n_tiles):
        store(t).wait()

    def take_cells(i, carry):
        owner(i).wait()
        return carry

    lax.fori_loop(1, count, take_cells, 0)
    sigma_ref[...] = jnp.sum(sig_recv[...], axis=0) + sig_send[me]


def solution(mesh):
    n_blk, n_pair = mesh.shape["blk"], mesh.shape["pair"]
    count = n_blk * n_pair

    def per_device(vertex, left_phase, right_phase, tiles, orders, momentum, frequency):
        height, breadth = vertex.shape[1], vertex.shape[2]
        states = right_phase.shape[2]
        n_tiles = tiles.shape[0]
        half = states // n_pair
        sizes = (n_blk, n_pair, height, breadth, states, n_tiles)
        bf16, f32 = jnp.bfloat16, jnp.float32
        dma = pltpu.SemaphoreType.DMA
        chi, cells = pl.pallas_call(
            lambda *refs: body(sizes, *refs),
            out_shape=(
                jax.ShapeDtypeStruct((n_tiles, half, states), bf16),
                jax.ShapeDtypeStruct((1, LANES), f32),
            ),
            in_specs=[
                pl.BlockSpec(memory_space=pltpu.SMEM),
                pl.BlockSpec(memory_space=pltpu.VMEM),
                pl.BlockSpec(memory_space=pltpu.VMEM),
            ] + [pl.BlockSpec(memory_space=pltpu.HBM)] * 4,
            out_specs=(
                pl.BlockSpec(memory_space=pltpu.HBM),
                pl.BlockSpec(memory_space=pltpu.VMEM),
            ),
            scratch_shapes=[
                pltpu.VMEM((height, breadth), bf16),
                pltpu.VMEM((height, states), bf16),
                pltpu.VMEM((SPLIT, breadth, states // SPLIT), bf16),
                pltpu.VMEM((n_tiles, states, states), bf16),
                pltpu.VMEM((height, states // SPLIT), bf16),
                pltpu.VMEM((states, states), f32),
                pltpu.VMEM((states, states), bf16),
                pltpu.VMEM((states, states), bf16),
                pltpu.VMEM((5, states, states), bf16),
                pltpu.VMEM((5, n_tiles * half, states), bf16),
                pltpu.VMEM((n_tiles * half, states), f32),
                pltpu.VMEM((NMOM, LANES), f32),
                pltpu.VMEM((count, 1, LANES), f32),
                pltpu.VMEM((count - 1, 1, LANES), f32),
                dma((SPLIT + 6,)),
            ] + [dma((CHUNKS,))] * 10 + [dma((count - 1,))] * 2 + [
                pltpu.VMEM((n_tiles, half, states), bf16), dma((n_tiles,))],
            compiler_params=pltpu.CompilerParams(
                collective_id=0, has_side_effects=True, vmem_limit_bytes=60 * 1024 * 1024
            ),
            name="measure_green",
        )(
            orders,
            momentum.reshape(n_pair, 1, half),
            frequency.reshape(1, states),
            vertex,
            left_phase,
            right_phase,
            tiles,
        )
        own = NMOM * NFREQ // count
        return chi, cells[0, :own]

    in_specs = (
        P("blk", "pair", None),
        P("blk", "pair", None),
        P("blk", None, None),
        P("blk", None, None),
        P("blk"),
        P(),
        P(),
    )
    out_specs = (P("blk", "pair", None), P(("blk", "pair")))
    return jax.shard_map(
        per_device, mesh=mesh, in_specs=in_specs, out_specs=out_specs, check_vma=False
    )
```

```python
import math

import jax
import jax.numpy as jnp
from jax import lax
from jax.experimental import pallas as pl
from jax.experimental.pallas import tpu as pltpu
from jax.sharding import PartitionSpec as P

NMOM = 64
NFREQ = 32
LANES = 128
CHUNKS = 4
SPLIT = 2
MESH = pl.DeviceIdType.MESH
OWN, PEER, ACROSS, RELAYED, FORWARDED = range(5)


def contract(a, b, dims, precision=None):
    return lax.dot_general(
        a, b, (dims, ((), ())), preferred_element_type=jnp.float32, precision=precision
    )


def body(sizes, order_ref, mom_ref, freq_ref, vertex_hbm, left_hbm, right_hbm, tiles_hbm,
         out_ref, sigma_ref,
         vertex, left, right, tiles, carried, partial, sending, arrived, greens, inner, acc,
         cells_ref, sig_send, sig_recv, load_sem, y_send, y_recv, x_send, x_recv, z_send, z_recv,
         p_send, p_recv, f_send, f_recv, s_send, s_recv,
         chi, o_sem):
    n_blk, n_pair, height, breadth, states, n_tiles = sizes
    count = n_blk * n_pair
    half = states // n_pair
    b = lax.axis_index("blk")
    p = lax.axis_index("pair")
    me = b * n_pair + p
    chip = b // 2
    core = lax.rem(b, 2)
    odd = lax.rem(chip, 2)
    step = 1 - 2 * odd
    across = (lax.rem(b + 2 * step + n_blk, n_blk), p)
    along = (lax.rem(b + 4 * step + n_blk, n_blk), p)
    peer = (b + 1 - 2 * core, p)
    other = (b, 1 - p)
    forwards_across = lax.rem(odd + core, 2) == 0

    barrier = pltpu.get_barrier_semaphore()

    def greet(i, carry):
        to = lax.rem(me + i, count)
        pl.semaphore_signal(barrier, inc=1, device_id=(to // n_pair, lax.rem(to, n_pair)),
                            device_id_type=MESH)
        return carry

    lax.fori_loop(1, count, greet, 0)

    pieces = 4
    block = height // pieces
    wide = states // SPLIT

    def load_right(h):
        cols = pl.ds(h * wide, wide)
        return pltpu.make_async_copy(right_hbm.at[0, :, cols], right.at[h], load_sem.at[h])

    load_right(0).start()
    load_vertex = []
    for i in range(pieces):
        rows = pl.ds(i * block, block)
        copy = pltpu.make_async_copy(vertex_hbm.at[0, rows], vertex.at[rows], load_sem.at[SPLIT + i])
        copy.start()
        load_vertex.append(copy)
    load_left = pltpu.make_async_copy(left_hbm.at[0], left, load_sem.at[SPLIT + pieces])
    load_left.start()
    for h in range(1, SPLIT):
        load_right(h).start()
    load_tiles = pltpu.make_async_copy(tiles_hbm, tiles, load_sem.at[SPLIT + 1 + pieces])
    load_tiles.start()

    order = order_ref[0]
    scale = 1.0 / math.sqrt(breadth)
    per_split = CHUNKS // SPLIT
    size = states // per_split
    per_half = half // size

    def chunk(which, k):
        index = lax.rem(which * per_half + k % per_split, per_split)
        return (pl.ds(pl.multiple_of(index * size, size), size),
                pl.ds(k // per_split * wide, wide))

    def exchange(k):
        rows = chunk(1 - p, k)
        return pltpu.make_async_remote_copy(
            src_ref=sending.at[*rows], dst_ref=arrived.at[*rows], send_sem=y_send.at[k],
            recv_sem=y_recv.at[k], device_id=other, device_id_type=MESH)

    def arrival(k):
        rows = chunk(p, k)
        return pltpu.make_async_remote_copy(
            src_ref=sending.at[*rows], dst_ref=arrived.at[*rows], send_sem=y_send.at[k],
            recv_sem=y_recv.at[k], device_id=other, device_id_type=MESH)

    def hop(source, target, k, send, recv, device):
        rows = chunk(p, k)
        return pltpu.make_async_remote_copy(
            src_ref=greens.at[source, *rows], dst_ref=greens.at[target, *rows], send_sem=send.at[k],
            recv_sem=recv.at[k], device_id=device, device_id_type=MESH)

    def to_across(k):
        return hop(OWN, ACROSS, k, x_send, x_recv, across)

    def to_peer(k):
        return hop(OWN, PEER, k, p_send, p_recv, peer)

    def to_along(k):
        return hop(ACROSS, RELAYED, k, z_send, z_recv, along)

    def forward(source, k):
        return hop(source, FORWARDED, k, f_send, f_recv, peer)

    for h in range(SPLIT):
        load_right(h).wait()

        def mask_right(i, carry):
            rows = pl.ds(pl.multiple_of(i * 256, 256), 256)
            ids = i * 256 + lax.broadcasted_iota(jnp.int32, (256, wide), 0)
            right[h, rows, :] = jnp.where(ids < order, right[h, rows, :], jnp.zeros((), jnp.bfloat16))
            return carry

        lax.fori_loop(0, breadth // 256, mask_right, 0)
        for i in range(pieces):
            rows = pl.ds(i * block, block)
            if h == 0:
                load_vertex[i].wait()
            product = contract(vertex[rows, :], right[h], ((1,), (0,)))
            ids = p * height + i * block + lax.broadcasted_iota(jnp.int32, (block, wide), 0)
            carried[rows, :] = jnp.where(ids < order, product, 0.0).astype(jnp.bfloat16)
        if h == 0:
            load_left.wait()
            pl.semaphore_wait(barrier, count - 1)
        cols = pl.ds(h * wide, wide)
        for part in range(n_pair):
            which = lax.rem(1 - p + part, n_pair)
            rows = pl.ds(pl.multiple_of(which * half, half), half)
            product = contract(left[:, rows], carried[...], ((0,), (0,))) * scale
            partial[rows, cols] = product
            sending[rows, cols] = product.astype(jnp.bfloat16)
            for k in range(per_half):
                exchange(h * per_split + part * per_half + k).start()

    ids_m = lax.broadcasted_iota(jnp.int32, (NMOM, half), 0)
    pick_mom = (ids_m == mom_ref[p]).astype(jnp.bfloat16)
    ids_f = lax.broadcasted_iota(jnp.int32, (LANES, states), 0)
    pick_freq = (ids_f == freq_ref[...]).astype(jnp.bfloat16)
    own_rows = pl.ds(pl.multiple_of(p * half, half), half)

    def compute_inner(slot, slot_index):
        upper = greens[slot, own_rows, :]
        total = jnp.zeros((half, states), jnp.float32)
        for t in range(n_tiles):
            value = contract(upper, tiles[t], ((1,), (0,))).astype(jnp.bfloat16)
            inner[slot_index, pl.ds(t * half, half), :] = value
            total = total + value.astype(jnp.float32)
        high = total.astype(jnp.bfloat16)
        low = (total - high.astype(jnp.float32)).astype(jnp.bfloat16)
        return contract(pick_mom, high, ((1,), (0,))) + contract(pick_mom, low, ((1,), (0,)))

    def compute_cells(slot, folded, first=False):
        picked = contract(pick_freq, greens[slot], ((1,), (0,)))
        value = contract(folded, picked, ((1,), (1,)), lax.Precision.HIGHEST)
        cells_ref[...] = value if first else cells_ref[...] + value

    out_scale = 1.0 / math.sqrt(states)

    def store(t):
        return pltpu.make_async_copy(chi.at[t], out_ref.at[t], o_sem.at[t])

    def compute_chi(slot, slot_index, first=False, last=False):
        for t in range(n_tiles):
            rows = pl.ds(t * half, half)
            value = contract(inner[slot_index, rows, :], greens[slot], ((1,), (1,)))
            if not first:
                value = acc[rows, :] + value
            if last:
                chi[t] = (value * out_scale).astype(jnp.bfloat16)
                store(t).start()
            else:
                acc[rows, :] = value

    def take_y(k):
        arrival(k).wait_recv()
        rows = chunk(p, k)
        greens[OWN, *rows] = (
            partial[*rows] + arrived[*rows].astype(jnp.float32)
        ).astype(jnp.bfloat16)
        to_across(k).start()
        to_peer(k).start()

    def take_x(k):
        to_across(k).wait_recv()
        to_along(k).start()

        @pl.when(forwards_across)
        def _():
            forward(ACROSS, k).start()

    def take_z(k):
        to_along(k).wait_recv()

        @pl.when(jnp.logical_not(forwards_across))
        def _():
            forward(RELAYED, k).start()

    folds = {}
    upper_last = CHUNKS - per_split + per_half - 1
    lag = 2
    for s in range(CHUNKS + 2 * lag):
        if s < CHUNKS:
            take_y(s)
        if 0 <= s - lag < CHUNKS:
            take_x(s - lag)
        if 0 <= s - 2 * lag < CHUNKS:
            take_z(s - 2 * lag)
        if s == upper_last:
            load_tiles.wait()
            folds[OWN] = compute_inner(OWN, 0)
        if s == CHUNKS - 1:
            compute_cells(OWN, folds[OWN], first=True)
            compute_chi(OWN, 0, first=True)
        if s == CHUNKS:
            for k in range(CHUNKS):
                to_peer(k).wait_recv()
            folds[PEER] = compute_inner(PEER, 1)
            folds[ACROSS] = compute_inner(ACROSS, 2)
        if s == CHUNKS + 1:
            compute_cells(PEER, folds[PEER])
            compute_cells(ACROSS, folds[ACROSS])
            compute_chi(PEER, 1)
        if s == CHUNKS + lag:
            folds[RELAYED] = compute_inner(RELAYED, 3)
            for k in range(upper_last + 1):
                forward(ACROSS, k).wait_recv()
            folds[FORWARDED] = compute_inner(FORWARDED, 4)

    compute_cells(RELAYED, folds[RELAYED])
    for k in range(upper_last + 1, CHUNKS):
        forward(ACROSS, k).wait_recv()
    compute_cells(FORWARDED, folds[FORWARDED])

    own_cells = NMOM * NFREQ // count
    cells = cells_ref[...]
    rows_d = lax.broadcasted_iota(jnp.int32, (count, NMOM), 0)
    cols_m = lax.broadcasted_iota(jnp.int32, (count, NMOM), 1)
    spread = jnp.zeros((count, LANES), jnp.float32)
    if own_cells >= NFREQ:
        group = own_cells // NFREQ
        for k in range(group):
            pick = (cols_m == rows_d * group + k).astype(jnp.float32)
            value = contract(pick, cells, ((1,), (0,)), lax.Precision.HIGHEST)
            spread = spread + (pltpu.roll(value, NFREQ * k, 1) if k else value)
    else:
        group = NFREQ // own_cells
        for k in range(group):
            pick = (rows_d == cols_m * group + k).astype(jnp.float32)
            value = contract(pick, cells, ((1,), (0,)), lax.Precision.HIGHEST)
            spread = spread + (pltpu.roll(value, LANES - own_cells * k, 1) if k else value)
    factor = 1.0 / math.sqrt(5.0 * n_tiles * n_blk * states * states / (NMOM * NFREQ))
    spread = spread * (factor * out_scale)
    sig_send[...] = spread.reshape(count, 1, LANES)

    def owner(i):
        to = lax.rem(me + i, count)
        return pltpu.make_async_remote_copy(
            src_ref=sig_send.at[to], dst_ref=sig_recv.at[i - 1], send_sem=s_send.at[i - 1],
            recv_sem=s_recv.at[i - 1], device_id=(to // n_pair, lax.rem(to, n_pair)),
            device_id_type=MESH)

    def send_cells(i, carry):
        owner(i).start()
        return carry

    lax.fori_loop(1, count, send_cells, 0)

    compute_chi(ACROSS, 2)
    compute_chi(RELAYED, 3)
    compute_chi(FORWARDED, 4, last=True)

    for k in range(CHUNKS):
        exchange(k).wait_send()
        to_across(k).wait_send()
        to_peer(k).wait_send()
        to_along(k).wait_send()
        forward(ACROSS, k).wait_send()

    for t in range(n_tiles):
        store(t).wait()

    def take_cells(i, carry):
        owner(i).wait()
        return carry

    lax.fori_loop(1, count, take_cells, 0)
    total = jnp.sum(sig_recv[...], axis=0) + sig_send[me]
    sigma_ref[...] = total[:, :own_cells]


def solution(mesh):
    n_blk, n_pair = mesh.shape["blk"], mesh.shape["pair"]
    count = n_blk * n_pair

    def per_device(vertex, left_phase, right_phase, tiles, orders, momentum, frequency):
        height, breadth = vertex.shape[1], vertex.shape[2]
        states = right_phase.shape[2]
        n_tiles = tiles.shape[0]
        half = states // n_pair
        sizes = (n_blk, n_pair, height, breadth, states, n_tiles)
        bf16, f32 = jnp.bfloat16, jnp.float32
        dma = pltpu.SemaphoreType.DMA
        chi, cells = pl.pallas_call(
            lambda *refs: body(sizes, *refs),
            out_shape=(
                jax.ShapeDtypeStruct((n_tiles, half, states), bf16),
                jax.ShapeDtypeStruct((1, NMOM * NFREQ // count), f32),
            ),
            in_specs=[
                pl.BlockSpec(memory_space=pltpu.SMEM),
                pl.BlockSpec(memory_space=pltpu.VMEM),
                pl.BlockSpec(memory_space=pltpu.VMEM),
            ] + [pl.BlockSpec(memory_space=pltpu.HBM)] * 4,
            out_specs=(
                pl.BlockSpec(memory_space=pltpu.HBM),
                pl.BlockSpec(memory_space=pltpu.VMEM),
            ),
            scratch_shapes=[
                pltpu.VMEM((height, breadth), bf16),
                pltpu.VMEM((height, states), bf16),
                pltpu.VMEM((SPLIT, breadth, states // SPLIT), bf16),
                pltpu.VMEM((n_tiles, states, states), bf16),
                pltpu.VMEM((height, states // SPLIT), bf16),
                pltpu.VMEM((states, states), f32),
                pltpu.VMEM((states, states), bf16),
                pltpu.VMEM((states, states), bf16),
                pltpu.VMEM((5, states, states), bf16),
                pltpu.VMEM((5, n_tiles * half, states), bf16),
                pltpu.VMEM((n_tiles * half, states), f32),
                pltpu.VMEM((NMOM, LANES), f32),
                pltpu.VMEM((count, 1, LANES), f32),
                pltpu.VMEM((count - 1, 1, LANES), f32),
                dma((SPLIT + 6,)),
            ] + [dma((CHUNKS,))] * 10 + [dma((count - 1,))] * 2 + [
                pltpu.VMEM((n_tiles, half, states), bf16), dma((n_tiles,))],
            compiler_params=pltpu.CompilerParams(
                collective_id=0, has_side_effects=True, vmem_limit_bytes=60 * 1024 * 1024
            ),
            name="measure_green",
        )(
            orders,
            momentum.reshape(n_pair, 1, half),
            frequency.reshape(1, states),
            vertex,
            left_phase,
            right_phase,
            tiles,
        )
        return chi, cells.reshape(-1)

    in_specs = (
        P("blk", "pair", None),
        P("blk", "pair", None),
        P("blk", None, None),
        P("blk", None, None),
        P("blk"),
        P(),
        P(),
    )
    out_specs = (P("blk", "pair", None), P(("blk", "pair")))
    return jax.shard_map(
        per_device, mesh=mesh, in_specs=in_specs, out_specs=out_specs, check_vma=False
    )
```
